32 devices in a mesh: rep: 1, dp: 32 (over x, y, z, core).
Axes of the slice: x: 2, y: 2, z: 4, core: 2. Of those that a mesh axis runs over, the one named last changes fastest.
Arguments:
- x: bfloat16 [32, 2048, 1024], P(('rep', 'dp'))
- dy: bfloat16 [32, 2048, 1024], P(('rep', 'dp'))
- w_gate: bfloat16 [2, 1024, 2816], replicated
- w_up: bfloat16 [2, 1024, 2816], replicated
- w_down: bfloat16 [2, 2816, 1024], replicated
- m_w_gate: float32 [2, 1024, 2816], replicated
- m_w_up: float32 [2, 1024, 2816], replicated
- m_w_down: float32 [2, 2816, 1024], replicated
- v_w_gate: float32 [2, 1024, 2816], replicated
- v_w_up: float32 [2, 1024, 2816], replicated
- v_w_down: float32 [2, 2816, 1024], replicated
Outputs:
- output 1: bfloat16 [2, 1024, 2816], P('rep')
- output 2: bfloat16 [2, 1024, 2816], P('rep')
- output 3: bfloat16 [2, 2816, 1024], P('rep')
- output 4: float32 [2, 1024, 2816], P('rep')
- output 5: float32 [2, 1024, 2816], P('rep')
- output 6: float32 [2, 2816, 1024], P('rep')
- output 7: float32 [2, 1024, 2816], P('rep')
- output 8: float32 [2, 1024, 2816], P('rep')
- output 9: float32 [2, 2816, 1024], P('rep')
All inputs are finite; a program needn't handle non-finite values.
Results may differ from the reference program's by a relative error of at most 0.022.
Values are sent between devices in bfloat16 or wider.
A program may use at most 2.75 GiB of HBM per device.

```python
import jax
import jax.numpy as jnp
from jax import lax

SEQUENCES = 32
TOKENS = 2048
D = 1024
FF = 2816
LAYERS = 2
NAMES = ("w_gate", "w_up", "w_down")
SHAPES = {"w_gate": (LAYERS, D, FF), "w_up": (LAYERS, D, FF), "w_down": (LAYERS, FF, D)}


def bump(key, n, height):
    away = (jnp.arange(n, dtype=jnp.int32) - jax.random.randint(key, (), 0, n, jnp.int32)) % n
    return jnp.where(away < n // 8, height, 1.0)


def together(key, own, strength):
    shared = jax.random.normal(key, own.shape[1:], jnp.float32)
    return (own + strength * shared) * lax.rsqrt(1 + strength * strength)


def setup_inputs(seed: int = 0, part: int = 0) -> dict:
    kx, kdy, ka, kb, kz, kf, kh, kl, *keys = jax.random.split(jax.random.key(seed), 8 + 3 * len(NAMES))
    kx, kdy, ka, kb = (jax.random.fold_in(k, part) for k in (kx, kdy, ka, kb))
    kw, km, kv = (keys[i::3] for i in range(3))
    shape = (SEQUENCES, TOKENS, D)
    much_x, much_dy = jax.random.uniform(kz, (2,), jnp.float32, 0.0, 1.0)
    loud = 2.0 ** jax.random.uniform(jax.random.fold_in(kz, 1), (), jnp.float32, -1.0, 2.0)
    layers = 2.0 ** jax.random.uniform(kl, (LAYERS, 1, 1), jnp.float32, -1.0, 1.0)
    x = together(ka, jax.random.normal(kx, shape, jnp.float32), much_x) * bump(kf, D, 4.0)
    dy = together(kb, jax.random.normal(kdy, shape, jnp.float32), much_dy)
    drawn = {"x": x.astype(jnp.bfloat16), "dy": (loud * dy * (SEQUENCES * TOKENS) ** -0.5).astype(jnp.bfloat16)}
    for key, name in zip(kw, NAMES, strict=True):
        w = jax.random.normal(key, SHAPES[name], jnp.float32) * SHAPES[name][1] ** -0.5
        drawn[name] = (w * {"w_gate": 1.0, "w_up": bump(kh, FF, 4.0), "w_down": layers}[name]).astype(jnp.bfloat16)
    for key, name in zip(km, NAMES, strict=True):
        drawn[f"m_{name}"] = 0.1 * jax.random.normal(key, SHAPES[name], jnp.float32)
    for key, name in zip(kv, NAMES, strict=True):
        drawn[f"v_{name}"] = jax.random.uniform(key, SHAPES[name], jnp.float32, 0.005, 0.015)
    return drawn


def matmul(a, w):
    return jnp.dot(a, w, preferred_element_type=jnp.float32).astype(jnp.bfloat16)


def normed(h):
    wide = h.astype(jnp.float32)
    scale = lax.rsqrt(jnp.mean(wide**2, -1, keepdims=True) + 1e-6)
    return (wide * scale).astype(jnp.bfloat16)


def layer(h, w):
    a = normed(h)
    gate = jnp.dot(a, w["w_gate"], preferred_element_type=jnp.float32)
    up = jnp.dot(a, w["w_up"], preferred_element_type=jnp.float32)
    return h + matmul((jax.nn.silu(gate) * up).astype(jnp.bfloat16), w["w_down"])


def adamw(w, m, v, g):
    m = 0.9 * m + 0.1 * g
    v = 0.95 * v + 0.05 * g * g
    step = m * lax.rsqrt(v + 1e-8) + 0.1 * w
    return (w - 0.02 * step).astype(jnp.bfloat16), m, v


def clipped(gradients, sum_of_squares, count):
    factor = jnp.minimum(1.0, 0.5 * lax.rsqrt(sum_of_squares / count + 1e-30))
    return [g * factor for g in gradients]


def stack(weights, h):
    return lax.scan(lambda h, w: (layer(h, w), None), h, weights)[0]


def reference(x, dy, w_gate, w_up, w_down, m_w_gate, m_w_up, m_w_down, v_w_gate, v_w_up, v_w_down):
    weights = dict(zip(NAMES, (w_gate, w_up, w_down), strict=True))

    def take(so_far, sequence):
        h, by_y = sequence
        _, back = jax.vjp(lambda w: stack(w, h), weights)
        return jax.tree.map(lambda total, term: total + term.astype(jnp.float32), so_far, back(by_y)[0]), None

    none_yet = {name: jnp.zeros(w.shape, jnp.float32) for name, w in weights.items()}
    by_weights, _ = lax.scan(take, none_yet, (x, dy))
    gradients = [by_weights[name].astype(jnp.bfloat16).astype(jnp.float32) for name in NAMES]
    gradients = clipped(gradients, sum(jnp.sum(g * g) for g in gradients), sum(g.size for g in gradients))
    new = [
        adamw(w.astype(jnp.float32), m, v, g)
        for w, m, v, g in zip((w_gate, w_up, w_down), (m_w_gate, m_w_up, m_w_down), (v_w_gate, v_w_up, v_w_down), gradients, strict=True)
    ]
    return tuple(one[which] for which in range(3) for one in new)
```

```python
import functools

import jax
import jax.numpy as jnp
from jax import lax
from jax.experimental import pallas as pl
from jax.experimental.pallas import tpu as pltpu
from jax.sharding import PartitionSpec as P

BF, F32 = jnp.bfloat16, jnp.float32
MiB = 2**20
ROWS = 256
CH = 256
STAGES = 4
ANY = pl.BlockSpec(memory_space=pl.ANY)
VMEM = pl.BlockSpec(memory_space=pltpu.VMEM)


def nn(a, b):
    return jnp.dot(a, b, preferred_element_type=F32)


def nt(a, b):
    return lax.dot_general(a, b, (((1,), (1,)), ((), ())), preferred_element_type=F32)


def normed(h):
    wide = h.astype(F32)
    scale = lax.rsqrt(jnp.mean(wide * wide, -1, keepdims=True) + 1e-6)
    return (wide * scale).astype(BF)


def gated(gate, up):
    sig = lax.logistic(gate)
    act = gate * sig
    return act * up, up * (sig + act * (1.0 - sig)), act


def weights_in(refs, bufs, sem):
    first = pl.program_id(0) == 0
    copies = [pltpu.make_async_copy(r, b, sem.at[i]) for i, (r, b) in enumerate(zip(refs, bufs, strict=True))]

    @pl.when(first)
    def _():
        for c in copies:
            c.start()

    def wait(i):
        @pl.when(first)
        def _():
            copies[i].wait()

    return wait


def forward_kernel(layer, x_ref, wg_hbm, wu_hbm, wd_hbm, s_ref, fa_ref, fb_ref, at_ref, h_ref, wg, wu, wd, sem):
    wait = weights_in([r.at[layer] for r in (wg_hbm, wu_hbm, wd_hbm)], (wg, wu, wd), sem)
    x = x_ref[0]
    a = normed(x)
    at_ref[...] = a.T
    wait(0)
    wait(1)
    for c in range(0, wg.shape[1], CH):
        cols = pl.ds(c, CH)
        prod, slope_g, slope_u = gated(nn(a, wg[:, cols]), nn(a, wu[:, cols]))
        s_ref[:, cols] = prod.astype(BF)
        fa_ref[:, cols] = slope_g
        fb_ref[:, cols] = slope_u
    wait(2)
    out = nn(s_ref[...], wd[...]).astype(BF)
    h_ref[...] = (x.astype(F32) + out.astype(F32)).astype(BF)


def top_kernel(layer, h_ref, dy_ref, wg_hbm, wu_hbm, wd_hbm, s_ref, dg_ref, du_ref, at_ref, dyt_ref, wg, wu, wd, sem):
    wait = weights_in([r.at[layer] for r in (wg_hbm, wu_hbm, wd_hbm)], (wg, wu, wd), sem)
    a = normed(h_ref[...])
    dy = dy_ref[0]
    at_ref[...] = a.T
    dyt_ref[...] = dy.T
    for i in range(3):
        wait(i)
    for c in range(0, wg.shape[1], CH):
        cols = pl.ds(c, CH)
        prod, slope_g, slope_u = gated(nn(a, wg[:, cols]), nn(a, wu[:, cols]))
        s_ref[:, cols] = prod.astype(BF)
        ds = nt(dy, wd[cols, :]).astype(BF).astype(F32)
        dg_ref[:, cols] = (ds * slope_g).astype(BF)
        du_ref[:, cols] = (ds * slope_u).astype(BF)


def between_kernel(layer, dg1_ref, du1_ref, h_ref, dy_ref, fa_ref, fb_ref, wg_hbm, wu_hbm, wd_hbm, dg_ref, du_ref, dht_ref, wg, wu, wd, sem):
    wait = weights_in([wg_hbm.at[layer + 1], wu_hbm.at[layer + 1], wd_hbm.at[layer]], (wg, wu, wd), sem)
    wait(0)
    by_gate = nt(dg1_ref[...], wg[...]).astype(BF).astype(F32)
    wait(1)
    by_up = nt(du1_ref[...], wu[...]).astype(BF).astype(F32)
    da = (by_gate + by_up).astype(BF).astype(F32)
    wide = h_ref[...].astype(F32)
    scale = lax.rsqrt(jnp.mean(wide * wide, -1, keepdims=True) + 1e-6)
    inner = jnp.mean(da * wide, -1, keepdims=True)
    dn = (da * scale - wide * (scale * scale * scale * inner)).astype(BF)
    dh = (dy_ref[0].astype(F32) + dn.astype(F32)).astype(BF)
    dht_ref[...] = dh.T
    wait(2)
    for c in range(0, wd.shape[0], CH):
        cols = pl.ds(c, CH)
        ds = nt(dh, wd[cols, :]).astype(BF).astype(F32)
        dg_ref[:, cols] = (ds * fa_ref[:, cols]).astype(BF)
        du_ref[:, cols] = (ds * fb_ref[:, cols]).astype(BF)


def row_local(kernel, name, ins, weights, outs, matmuls):
    tokens, d, ff = 2048, weights[0].shape[1], weights[0].shape[2]

    def spec(a):
        if len(a.shape) == 3:
            return pl.BlockSpec((1, ROWS, a.shape[2]), lambda i: (0, i, 0))
        if a.shape[1] == tokens:
            return pl.BlockSpec((a.shape[0], ROWS), lambda i: (0, i))
        return pl.BlockSpec((ROWS, a.shape[1]), lambda i: (i, 0))

    return pl.pallas_call(
        kernel,
        grid=(tokens // ROWS,),
        in_specs=[spec(a) for a in ins] + [ANY] * 3,
        out_specs=[spec(a) for a in outs],
        out_shape=outs,
        scratch_shapes=[pltpu.VMEM((d, ff), BF), pltpu.VMEM((d, ff), BF), pltpu.VMEM((ff, d), BF), pltpu.SemaphoreType.DMA((3,))],
        compiler_params=pltpu.CompilerParams(dimension_semantics=("arbitrary",), vmem_limit_bytes=62 * MiB),
        cost_estimate=pl.CostEstimate(flops=matmuls * 2 * tokens * d * ff, bytes_accessed=8 * tokens * ff, transcendentals=0),
        name=name,
    )(*ins, *weights)


def struct(dtype, *shape):
    return jax.ShapeDtypeStruct(shape, dtype)


def colour(c):
    late = c % 9
    along_z = (late == 4) | (late == 8)
    return jnp.where(along_z, 2, c % 2)


def bit_of(stage, c):
    if stage == 0:
        return 1
    k = colour(c)
    x, y, z = ((16, 8, 2, 4)[stage - 1], (8, 16, 2, 4)[stage - 1], (2, 4, 16, 8)[stage - 1])
    return jnp.where(k == 2, z, jnp.where(k == 0, x, y))


def side_of(me, bit):
    return (me // bit) % 2


def partner_of(me, bit):
    return me + bit - 2 * bit * side_of(me, bit)


def rows_of(device, c):
    at = side_of(device, 1) * 512
    for k in range(1, STAGES + 1):
        at = at + side_of(device, bit_of(k, c)) * (512 >> k)
    return at


def mult(x, m):
    return pl.multiple_of(x, m)


def reduce_kernel(n, per, lags, lhs_d, lhs_g, s_ref, dg_ref, du_ref, own_ref, sq_ref,
                  lhs, rhs, acc, send0, recv0, bufs_s, bufs_r, lhs_sem, rhs_sem, ssem0, rsem0, ssem, rsem):
    me = lax.axis_index("dp")
    total = 3 * per
    half = 512
    core = side_of(me, 1)

    def rhs_start(c):
        for which, ref in enumerate((s_ref, dg_ref, du_ref)):
            @pl.when((c >= which * per) & (c < (which + 1) * per))
            def _():
                cols = pl.ds(mult((c - which * per) * CH, CH), CH)
                pltpu.make_async_copy(ref.at[:, cols], rhs.at[c % 3], rhs_sem.at[c % 3]).start()

    def rhs_wait(c):
        pltpu.make_async_copy(s_ref.at[:, pl.ds(0, CH)], rhs.at[c % 3], rhs_sem.at[c % 3]).wait()

    def core_copy(c):
        return pltpu.make_async_remote_copy(send0.at[c % 4], recv0.at[c], ssem0.at[c % 4], rsem0.at[c],
                                            device_id={"dp": partner_of(me, 1)}, device_id_type=pl.DeviceIdType.MESH)

    def stage_copy(k, c):
        return pltpu.make_async_remote_copy(bufs_s[k - 1].at[c], bufs_r[k - 1].at[c], ssem.at[k - 1, c], rsem.at[k - 1, c],
                                            device_id={"dp": partner_of(me, bit_of(k, c))}, device_id_type=pl.DeviceIdType.MESH)

    cps = [pltpu.make_async_copy(lhs_d, lhs.at[0], lhs_sem.at[0]), pltpu.make_async_copy(lhs_g, lhs.at[1], lhs_sem.at[1])]
    cps[0].start()
    rhs_start(0)
    rhs_start(1)
    cps[1].start()
    cps[0].wait()
    cps[1].wait()
    sq_ref[...] = jnp.zeros_like(sq_ref)

    def compute(c):
        rhs_wait(c)
        @pl.when(c + 2 < total)
        def _():
            rhs_start(c + 2)
        @pl.when(c >= 4)
        def _():
            core_copy(c - 4).wait_send()
        which = jnp.where(c < per, 0, 1)
        b = rhs[c % 3]
        send0[c % 4] = jnp.dot(lhs[which, pl.ds(mult((1 - core) * half, half), half), :], b, preferred_element_type=F32).astype(BF)
        acc[c] = jnp.dot(lhs[which, pl.ds(mult(core * half, half), half), :], b, preferred_element_type=F32)
        core_copy(c).start()

    def offset(k, c):
        at = 0
        for s in range(1, k + 1):
            at = at + side_of(me, bit_of(s, c)) * (half >> s)
        return at

    def stage_job(k, c):
        if k == 0:
            core_copy(c).wait_recv()
            got = recv0
        else:
            stage_copy(k, c).wait_recv()
            got = bufs_r[k - 1]
        base = offset(k, c)
        rows = half >> k
        if k == STAGES:
            out = (acc[c, pl.ds(mult(base, rows), rows), :] + got[c].astype(F32)).astype(BF)
            own_ref[c] = out
            wide = out.astype(F32)
            sq_ref[...] += wide * wide
            return
        n2 = rows // 2
        side = side_of(me, bit_of(k + 1, c))
        ds, dk = mult((1 - side) * n2, n2), mult(side * n2, n2)
        bufs_s[k][c] = (acc[c, pl.ds(mult(base + ds, n2), n2), :] + got[c, pl.ds(ds, n2), :].astype(F32)).astype(BF)
        stage_copy(k + 1, c).start()
        acc[c, pl.ds(mult(base + dk, n2), n2), :] += got[c, pl.ds(dk, n2), :].astype(F32)

    lag0, *later = lags
    steps = total + later[-1]

    def step(i, _):
        @pl.when(i < total)
        def _():
            compute(i)
        @pl.when((i >= lag0) & (i < total + lag0))
        def _():
            stage_job(0, i - lag0)
        for k in range(1, STAGES + 1):
            c = i - later[k - 1]
            @pl.when((c >= 0) & (c < total))
            def _():
                stage_job(k, c)
        return 0

    lax.fori_loop(0, steps, step, 0)

    def settle(c, _):
        for k in range(1, STAGES + 1):
            stage_copy(k, c).wait_send()
        return 0

    lax.fori_loop(0, total, settle, 0)
    for c in range(total - 4, total):
        core_copy(c).wait_send()


def entry(fn):
    def wrapped(*refs):
        me = lax.axis_index("dp")
        barrier = pltpu.get_barrier_semaphore()
        for bit in (1, 2, 4, 8, 16):
            pl.semaphore_signal(barrier, inc=1, device_id={"dp": partner_of(me, bit)}, device_id_type=pl.DeviceIdType.MESH)
        pl.semaphore_wait(barrier, 5)
        fn(*refs)
    return wrapped


def reduced(lhs_d, lhs_g, s, dg, du, cid, lags=(2, 6, 10, 14, 18)):
    n = 32
    per = s.shape[1] // CH
    total = 3 * per
    T = s.shape[0]

    def body(a, b, c, d, e, own, sq, lhs, rhs, acc, send0, recv0, s1, s2, s3, s4, r1, r2, r3, r4, *sems):
        reduce_kernel(n, per, lags, a, b, c, d, e, own, sq, lhs, rhs, acc, send0, recv0, (s1, s2, s3, s4), (r1, r2, r3, r4), *sems)

    return pl.pallas_call(
        entry(body),
        out_shape=(jax.ShapeDtypeStruct((total, 32, CH), BF), jax.ShapeDtypeStruct((32, CH), F32)),
        in_specs=[ANY] * 5,
        out_specs=(VMEM, VMEM),
        scratch_shapes=[
            pltpu.VMEM((2, 1024, T), BF),
            pltpu.VMEM((3, T, CH), BF),
            pltpu.VMEM((total, 512, CH), F32),
            pltpu.VMEM((4, 512, CH), BF),
            pltpu.VMEM((total, 512, CH), BF),
            *[pltpu.VMEM((total, 512 >> k, CH), BF) for k in range(1, STAGES + 1)] * 2,
            pltpu.SemaphoreType.DMA((2,)),
            pltpu.SemaphoreType.DMA((3,)),
            pltpu.SemaphoreType.DMA((4,)),
            pltpu.SemaphoreType.DMA((total,)),
            pltpu.SemaphoreType.DMA((STAGES, total)),
            pltpu.SemaphoreType.DMA((STAGES, total)),
        ],
        compiler_params=pltpu.CompilerParams(collective_id=cid, has_side_effects=True, vmem_limit_bytes=63 * MiB),
        cost_estimate=pl.CostEstimate(flops=3 * 2 * T * 1024 * s.shape[1], bytes_accessed=3 * 2 * T * s.shape[1], transcendentals=0),
        name=f"reduce{cid}",
    )(lhs_d, lhs_g, s, dg, du)


def adam_kernel(layer, matrix, per, flip, factor_ref, g_ref, w_ref, m_ref, v_ref, *rest):
    *_, wo_ref, mo_ref, vo_ref, gt = rest
    c = matrix * per + pl.program_id(0)
    factor = factor_ref[0, 0]

    def update(at, g):
        g = g * factor
        m = 0.9 * m_ref[at] + 0.1 * g
        v = 0.95 * v_ref[at] + 0.05 * g * g
        w = w_ref[at].astype(F32)
        wo_ref[at] = (w - 0.02 * (m * lax.rsqrt(v + 1e-8) + 0.1 * w)).astype(BF)
        mo_ref[at] = m
        vo_ref[at] = v

    for device in range(32):
        base = rows_of(device, c)
        if flip:
            gt[pl.ds(mult(base, 32), 32), :] = g_ref[device, 0].astype(F32)
        else:
            update((0, pl.ds(mult(base, 32), 32), slice(None)), g_ref[device, 0].astype(F32))
    if flip:
        for q in range(0, 1024, 128):
            update((0, slice(None), pl.ds(q, 128)), gt[pl.ds(q, 128), :].T)


def adam(layer, matrix, flip, factor, g, w, m, v, before):
    layers, rows, columns = w.shape
    per = (rows if flip else columns) // CH
    if flip:
        block = pl.BlockSpec((1, CH, columns), lambda j: (layer, j, 0))
    else:
        block = pl.BlockSpec((1, rows, CH), lambda j: (layer, 0, j))
    before = before or ()
    return pl.pallas_call(
        functools.partial(adam_kernel, layer, matrix, per, flip),
        grid=(per,),
        in_specs=[
            pl.BlockSpec(memory_space=pltpu.SMEM),
            pl.BlockSpec((32, 1, 32, CH), lambda j: (0, matrix * per + j, 0, 0)),
            block, block, block, *[ANY] * len(before),
        ],
        out_specs=[block] * 3,
        out_shape=(struct(BF, *w.shape), struct(F32, *w.shape), struct(F32, *w.shape)),
        scratch_shapes=[pltpu.VMEM((1024, CH), F32)],
        input_output_aliases={5 + i: i for i in range(len(before))},
        compiler_params=pltpu.CompilerParams(dimension_semantics=("arbitrary",), vmem_limit_bytes=48 * MiB),
        cost_estimate=pl.CostEstimate(flops=10 * rows * columns, bytes_accessed=22 * rows * columns, transcendentals=rows * columns),
        name=f"adam{layer}{matrix}",
    )(factor, g, w, m, v, *before)


def solution(mesh):
    def step(x, dy, *arrays):
        weights, m, v = (arrays[i : i + 3] for i in (0, 3, 6))
        layers, d, ff = weights[0].shape
        t = x.shape[1]
        wide, tall, flat = struct(BF, t, ff), struct(BF, d, t), struct(BF, t, d)
        s0, fa, fb, a0t, h1 = row_local(functools.partial(forward_kernel, 0), "fwd0", [x], weights,
                                        [wide, struct(F32, t, ff), struct(F32, t, ff), tall, flat], 3)
        s1, dg1, du1, a1t, dyt = row_local(functools.partial(top_kernel, 1), "top", [h1, dy], weights, [wide, wide, wide, tall, tall], 3)
        own1, sq1 = reduced(dyt, a1t, s1, dg1, du1, 1)
        dg0, du0, dht = row_local(functools.partial(between_kernel, 0), "between", [dg1, du1, h1, dy, fa, fb], weights, [wide, wide, tall], 3)
        own0, sq0 = reduced(dht, a0t, s0, dg0, du0, 2)
        squares = lax.psum(jnp.sum(sq1) + jnp.sum(sq0), "dp")
        count = 3 * layers * d * ff
        factor = jnp.minimum(1.0, 0.5 * lax.rsqrt(squares / count + 1e-30)).reshape(1, 1)
        g1 = lax.all_gather(own1, "dp")
        g0 = lax.all_gather(own0, "dp")
        new = {}
        for name, which, matrix, flip in ((2, 2, 0, True), (0, 0, 1, False), (1, 1, 2, False)):
            new[name] = adam(1, matrix, flip, factor, g1, weights[which], m[which], v[which], None)
        for name, which, matrix, flip in ((2, 2, 0, True), (0, 0, 1, False), (1, 1, 2, False)):
            new[name] = adam(0, matrix, flip, factor, g0, weights[which], m[which], v[which], new[name])
        return tuple(new[i][which] for which in range(3) for i in range(3))

    return jax.shard_map(
        step,
        mesh=mesh,
        in_specs=(P(("rep", "dp"), None, None),) * 2 + (P(None, None, None),) * 9,
        out_specs=(P("rep", None, None),) * 9,
        check_vma=False,
    )
```

```python
import functools

import jax
import jax.numpy as jnp
from jax import lax
from jax.experimental import pallas as pl
from jax.experimental.pallas import tpu as pltpu
from jax.sharding import PartitionSpec as P

BF, F32 = jnp.bfloat16, jnp.float32
MiB = 2**20
ROWS = 256
CH = 256
STAGES = 4
ANY = pl.BlockSpec(memory_space=pl.ANY)
VMEM = pl.BlockSpec(memory_space=pltpu.VMEM)
COUNT = 6 * 1024 * 2816
FLOPS_PER_CHUNK = 800_000_000


def loop(first, stop, do):
    def step(i, carry):
        do(i)
        return carry

    lax.fori_loop(first, stop, step, 0)


def nn(a, b):
    return jnp.dot(a, b, preferred_element_type=F32)


def nt(a, b):
    return lax.dot_general(a, b, (((1,), (1,)), ((), ())), preferred_element_type=F32)


def normed(h):
    wide = h.astype(F32)
    scale = lax.rsqrt(jnp.mean(wide * wide, -1, keepdims=True) + 1e-6)
    return (wide * scale).astype(BF)


def gated(gate, up):
    sig = lax.logistic(gate)
    act = gate * sig
    return act * up, up * (sig + act * (1.0 - sig)), act


def weights_in(refs, bufs, sem):
    first = pl.program_id(0) == 0
    copies = [pltpu.make_async_copy(r, b, sem.at[i]) for i, (r, b) in enumerate(zip(refs, bufs, strict=True))]

    @pl.when(first)
    def _():
        for c in copies:
            c.start()

    def wait(i):
        @pl.when(first)
        def _():
            copies[i].wait()

    return wait


def forward_kernel(layer, x_ref, wg_hbm, wu_hbm, wd_hbm, s_ref, fa_ref, fb_ref, at_ref, h_ref, wg, wu, wd, sem):
    wait = weights_in([r.at[layer] for r in (wg_hbm, wu_hbm, wd_hbm)], (wg, wu, wd), sem)
    x = x_ref[0]
    a = normed(x)
    at_ref[...] = a.T
    wait(0)
    wait(1)
    for c in range(0, wg.shape[1], CH):
        cols = pl.ds(c, CH)
        prod, slope_g, slope_u = gated(nn(a, wg[:, cols]), nn(a, wu[:, cols]))
        s_ref[:, cols] = prod.astype(BF)
        fa_ref[:, cols] = slope_g
        fb_ref[:, cols] = slope_u
    wait(2)
    out = nn(s_ref[...], wd[...]).astype(BF)
    h_ref[...] = (x.astype(F32) + out.astype(F32)).astype(BF)


def top_kernel(layer, h_ref, dy_ref, wg_hbm, wu_hbm, wd_hbm, s_ref, dg_ref, du_ref, at_ref, dyt_ref, wg, wu, wd, sem):
    wait = weights_in([r.at[layer] for r in (wg_hbm, wu_hbm, wd_hbm)], (wg, wu, wd), sem)
    a = normed(h_ref[...])
    dy = dy_ref[0]
    at_ref[...] = a.T
    dyt_ref[...] = dy.T
    for i in range(3):
        wait(i)
    for c in range(0, wg.shape[1], CH):
        cols = pl.ds(c, CH)
        prod, slope_g, slope_u = gated(nn(a, wg[:, cols]), nn(a, wu[:, cols]))
        s_ref[:, cols] = prod.astype(BF)
        ds = nt(dy, wd[cols, :]).astype(BF).astype(F32)
        dg_ref[:, cols] = (ds * slope_g).astype(BF)
        du_ref[:, cols] = (ds * slope_u).astype(BF)


def struct(dtype, *shape):
    return jax.ShapeDtypeStruct(shape, dtype)


def row_local(kernel, name, ins, weights, outs, matmuls, whole=(), free=(), scratch=(), cid=None):
    tokens, d, ff = 2048, weights[0].shape[1], weights[0].shape[2]

    def spec(a):
        if len(a.shape) == 3:
            return pl.BlockSpec((1, ROWS, a.shape[2]), lambda i: (0, i, 0))
        if a.shape[1] == tokens:
            return pl.BlockSpec((a.shape[0], ROWS), lambda i: (0, i))
        return pl.BlockSpec((ROWS, a.shape[1]), lambda i: (i, 0))

    return pl.pallas_call(
        kernel,
        grid=(tokens // ROWS,),
        in_specs=[spec(a) for a in ins] + [VMEM] * len(whole) + [ANY] * 3,
        out_specs=[spec(a) for a in outs] + [ANY if len(a.shape) == 3 else VMEM for a in free],
        out_shape=[*outs, *free],
        scratch_shapes=[pltpu.VMEM((d, ff), BF), pltpu.VMEM((d, ff), BF), pltpu.VMEM((ff, d), BF), pltpu.SemaphoreType.DMA((3,)), *scratch],
        compiler_params=pltpu.CompilerParams(dimension_semantics=("arbitrary",), vmem_limit_bytes=63 * MiB, collective_id=cid, has_side_effects=cid is not None),
        cost_estimate=pl.CostEstimate(flops=matmuls * 2 * tokens * d * ff, bytes_accessed=8 * tokens * ff, transcendentals=0),
        name=name,
    )(*ins, *whole, *weights)


CHUNKS = 33
KINDS = (0, 14, 28, 33)
MESH = pl.DeviceIdType.MESH
LAGS = (6, 10, 14, 18, 21)
BEHIND = 2


def in_order(i):
    return (13 * i) % CHUNKS


def bit_of(stage, c):
    if stage == 0:
        return 1
    x, y, z = ((16, 8, 2, 4)[stage - 1], (8, 16, 2, 4)[stage - 1], (2, 4, 16, 8)[stage - 1])
    if x == y == z:
        return x
    return jnp.where(c < KINDS[1], x, jnp.where(c < KINDS[2], y, z))


def side_of(me, bit):
    return (me // bit) % 2


def partner_of(me, bit):
    return me + bit - 2 * bit * side_of(me, bit)


def mult(x, m):
    return pl.multiple_of(x, m)


def offset(me, k, c):
    at = 0
    for s in range(1, k + 1):
        at = at + side_of(me, bit_of(s, c)) * (512 >> s)
    return at


def meet(me, everyone):
    barrier = pltpu.get_barrier_semaphore()
    if everyone:
        def signal(d):
            pl.semaphore_signal(barrier, inc=1, device_id={"dp": (me + d) % 32}, device_id_type=MESH)
        loop(1, 32, signal)
        pl.semaphore_wait(barrier, 31)
    else:
        for bit in (1, 2, 4, 8, 16):
            pl.semaphore_signal(barrier, inc=1, device_id={"dp": partner_of(me, bit)}, device_id_type=MESH)
        pl.semaphore_wait(barrier, 5)


def squares_of(sums):
    return sum(sums[r : r + 8, q : q + 128] for r in range(0, 32, 8) for q in range(0, CH, 128))


def halves(me, k, c):
    n = 256 >> k
    side = side_of(me, bit_of(k + 1, c))
    return pl.ds(mult((1 - side) * n, n), n), pl.ds(mult(side * n, n), n)


def partner(me, stage, c):
    return dict(device_id={"dp": partner_of(me, bit_of(stage, c))}, device_id_type=MESH)


def produce(me, lhs_refs, rhs_refs, bufs, sems, stage1, jobs, stop, meeting):
    lhs, rhs, send0, recv0, s1, kept = bufs
    lhs_sem, rhs_sem, ssem0, rsem0 = sems
    per = CHUNKS // 3
    core = side_of(me, 1)

    def rhs_copy(i, act):
        c = in_order(i)
        for which, ref in enumerate(rhs_refs):
            @pl.when(c // per == which)
            def _():
                cols = pl.ds(mult((c - which * per) * CH, CH), CH)
                getattr(pltpu.make_async_copy(ref.at[:, cols], rhs.at[i % 5], rhs_sem.at[i % 5]), act)()

    def core_copy(i):
        return pltpu.make_async_remote_copy(send0.at[i % 4], recv0.at[i], ssem0.at[i % 4], rsem0.at[i], **partner(me, 0, 0))

    cps = [pltpu.make_async_copy(ref, lhs.at[j], lhs_sem.at[j]) for j, ref in enumerate(lhs_refs)]
    cps[0].start()
    rhs_copy(0, "start")
    cps[1].start()
    rhs_copy(1, "start")
    meet(me, meeting)
    cps[0].wait()
    cps[1].wait()

    def product(i, row, rows):
        which = jnp.where(in_order(i) < per, 0, 1)
        return nn(lhs[which, pl.ds(mult(row, rows), rows), :], rhs[i % 5])

    def step(theirs, ours, i):
        j = i - BEHIND
        if theirs:
            rhs_copy(i, "wait")

            @pl.when(i + 2 < CHUNKS)
            def _():
                rhs_copy(i + 2, "start")

            @pl.when(i >= 4)
            def _():
                core_copy(i - 4).wait_send()
        if ours:
            core_copy(j).wait_recv()
            side = side_of(me, bit_of(1, in_order(j)))
            give, keep = (1 - side) * 256, side * 256
        if theirs:
            send0[i % 4] = product(i, (1 - core) * 512, 512).astype(BF)
        if ours:
            s1[j] = (product(j, core * 512 + give, 256) + recv0[j, pl.ds(mult(give, 256), 256), :].astype(F32)).astype(BF)
            kept[j] = product(j, core * 512 + keep, 256) + recv0[j, pl.ds(mult(keep, 256), 256), :].astype(F32)
        if theirs:
            core_copy(i).start()
        if ours:
            stage1(j).start()
        for lag, job in jobs:
            @pl.when((i >= lag) & (i < CHUNKS + lag))
            def _():
                job(i - lag)

    loop(0, BEHIND, functools.partial(step, True, False))
    loop(BEHIND, CHUNKS, functools.partial(step, True, True))
    loop(CHUNKS, CHUNKS + BEHIND, functools.partial(step, False, True))
    loop(CHUNKS + BEHIND, stop, functools.partial(step, False, False))
    for i in range(CHUNKS - 4, CHUNKS):
        core_copy(i).wait_send()


def produce_scratch(t):
    bufs = [
        pltpu.VMEM((2, 1024, t), BF),
        pltpu.VMEM((5, t, CH), BF),
        pltpu.VMEM((4, 512, CH), BF),
        pltpu.VMEM((CHUNKS, 512, CH), BF),
        pltpu.VMEM((CHUNKS, 256, CH), BF),
        pltpu.VMEM((CHUNKS, 256, CH), F32),
    ]
    sems = [pltpu.SemaphoreType.DMA((n,)) for n in (2, 5, 4, CHUNKS)]
    return bufs, sems


def begin_kernel(lhs_d, lhs_g, s_ref, dg_ref, du_ref, give_ref, keep_ref, *refs):
    bufs, (r1, *sems, ssem, rsem) = refs[:6], refs[6:]
    me = lax.axis_index("dp")
    s1, kept = bufs[4:]

    def stage1(i):
        return pltpu.make_async_remote_copy(s1.at[i], r1.at[i], ssem.at[i], rsem.at[i], **partner(me, 1, in_order(i)))

    def job(i):
        give, keep = halves(me, 1, in_order(i))
        stage1(i).wait_recv()
        give_ref[i] = (kept[i, give, :] + r1[i, give, :].astype(F32)).astype(BF)
        keep_ref[i] = kept[i, keep, :] + r1[i, keep, :].astype(F32)

    produce(me, (lhs_d, lhs_g), (s_ref, dg_ref, du_ref), bufs, sems, stage1, [(LAGS[0], job)], CHUNKS + LAGS[0], False)

    def settle(i):
        stage1(i).wait_send()
    loop(0, CHUNKS, settle)


def cost(t, d, ff):
    return pl.CostEstimate(flops=3 * 2 * t * d * ff, bytes_accessed=3 * 2 * t * ff, transcendentals=0)


def begun(lhs_d, lhs_g, s, dg, du, cid):
    t = s.shape[0]
    bufs, sems = produce_scratch(t)
    return pl.pallas_call(
        begin_kernel,
        out_shape=[struct(BF, CHUNKS, 128, CH), struct(F32, CHUNKS, 128, CH)],
        in_specs=[ANY] * 5,
        out_specs=[VMEM] * 2,
        scratch_shapes=[*bufs, pltpu.VMEM((CHUNKS, 256, CH), BF), *sems, pltpu.SemaphoreType.DMA((CHUNKS,)), pltpu.SemaphoreType.DMA((CHUNKS,))],
        compiler_params=pltpu.CompilerParams(collective_id=cid, has_side_effects=True, vmem_limit_bytes=63 * MiB),
        cost_estimate=cost(t, 1024, s.shape[1]),
        name="begin",
    )(lhs_d, lhs_g, s, dg, du)


def whole_kernel(lhs_d, lhs_g, s_ref, dg_ref, du_ref, sq1, *refs):
    outs, total_ref, refs = refs[:3], refs[3], refs[4:]
    bufs, refs = refs[:6], refs[6:]
    s1, kept = bufs[4:]
    sends, recvs, refs = (s1, *refs[:3]), refs[3:7], refs[7:]
    sq_ref, near, squares, *sems = refs
    sems, (ssem, rsem, gsem_s, gsem_r, sq_sem, out_sem) = sems[:4], sems[4:]
    me = lax.axis_index("dp")

    def stage_copy(k, i):
        return pltpu.make_async_remote_copy(sends[k - 1].at[i], recvs[k - 1].at[i], ssem.at[k - 1, i], rsem.at[k - 1, i], **partner(me, k, in_order(i)))

    def gather_copy(k, i):
        c = in_order(i)
        rows = pl.ds(mult(offset(me, k, c) - offset(me, 2, c), 512 >> k), 512 >> k)
        return pltpu.make_async_remote_copy(near.at[c, rows], near.at[c, rows], gsem_s.at[k - 3, i], gsem_r.at[k - 3, i], **partner(me, k, c))

    def stage_job(k, i):
        c = in_order(i)
        stage_copy(k, i).wait_recv()
        got = recvs[k - 1]
        base = mult(offset(me, k, c) - offset(me, 1, c), 512 >> k)
        if k == STAGES:
            out = (kept[i, pl.ds(base, 32), :] + got[i].astype(F32)).astype(BF)
            wide = out.astype(F32)
            sq_ref[...] += wide * wide
            near[c, pl.ds(mult(base - (offset(me, 2, c) - offset(me, 1, c)), 32), 32), :] = out
            gather_copy(STAGES, i).start()
            return
        give, keep = halves(me, k, c)
        n = 256 >> k
        sends[k][i] = (kept[i, pl.ds(mult(base + give.start, n), n), :] + got[i, give, :].astype(F32)).astype(BF)
        stage_copy(k + 1, i).start()
        kept[i, pl.ds(mult(base + keep.start, n), n), :] += got[i, keep, :].astype(F32)

    def gather_job(k, i):
        gather_copy(k, i).wait_recv()
        if k > 3:
            gather_copy(k - 1, i).start()

    jobs = [functools.partial(stage_job, k) for k in range(1, STAGES + 1)] + [functools.partial(gather_job, STAGES)]
    sq_ref[...] = jnp.zeros_like(sq_ref)
    produce(me, (lhs_d, lhs_g), (s_ref, dg_ref, du_ref), bufs, sems, functools.partial(stage_copy, 1), list(zip(LAGS, jobs)), CHUNKS + LAGS[-2], True)
    squares[me] = squares_of(sq_ref) + sq1[...]

    def tell(d):
        pltpu.make_async_remote_copy(squares.at[me], squares.at[me], sq_sem.at[0], sq_sem.at[1],
                                     device_id={"dp": (me + d) % 32}, device_id_type=MESH).start()
    loop(1, 32, tell)

    def rest(i):
        gather_job(STAGES, i)
    loop(CHUNKS + LAGS[-2] - LAGS[-1], CHUNKS, rest)

    def settle(i):
        gather_job(3, i)
        for k in range(1, STAGES + 1):
            stage_copy(k, i).wait_send()
        for k in range(3, STAGES + 1):
            gather_copy(k, i).wait_send()
    loop(0, CHUNKS, settle)
    copies = [pltpu.make_async_copy(near.at[pl.ds(a, b - a)], g, out_sem.at[j]) for j, (a, b, g) in enumerate(zip(KINDS, KINDS[1:], outs))]
    for o in copies:
        o.start()
    all_but_one = squares.at[pl.ds(0, 31)]
    pltpu.make_async_copy(all_but_one, all_but_one, sq_sem.at[0]).wait()
    pltpu.make_async_copy(all_but_one, all_but_one, sq_sem.at[1]).wait()
    total_ref[...] = functools.reduce(jnp.add, [squares[d] for d in range(32)])
    for o in copies:
        o.wait()


def by_kind(rows):
    return [struct(BF, b - a, rows, CH) for a, b in zip(KINDS, KINDS[1:])]


def summed(lhs_d, lhs_g, s, dg, du, sq1, cid):
    t = s.shape[0]
    bufs, sems = produce_scratch(t)
    return pl.pallas_call(
        whole_kernel,
        out_shape=[*by_kind(128), struct(F32, 8, 128)],
        in_specs=[ANY] * 5 + [VMEM],
        out_specs=[ANY] * 3 + [VMEM],
        scratch_shapes=[
            *bufs,
            *[pltpu.VMEM((CHUNKS, 512 >> k, CH), BF) for k in (2, 3, 4, 1, 2, 3, 4)],
            pltpu.VMEM((32, CH), F32),
            pltpu.VMEM((CHUNKS, 128, CH), BF),
            pltpu.VMEM((32, 8, 128), F32),
            *sems,
            *[pltpu.SemaphoreType.DMA((n, CHUNKS)) for n in (STAGES, STAGES, 2, 2)],
            pltpu.SemaphoreType.DMA((2,)),
            pltpu.SemaphoreType.DMA((3,)),
        ],
        compiler_params=pltpu.CompilerParams(collective_id=cid, has_side_effects=True, vmem_limit_bytes=63 * MiB),
        cost_estimate=cost(t, 1024, s.shape[1]),
        name="whole",
    )(lhs_d, lhs_g, s, dg, du, sq1)


POINTS = 4
RATE = 2
POINT_LAGS = (1, 4, 7, 9, 11, 13)


def between_kernel(layer, dg1_ref, du1_ref, h_ref, dy_ref, fa_ref, fb_ref, s2, kept2, wg_hbm, wu_hbm, wd_hbm,
                   dg_ref, du_ref, dht_ref, gx, gy, gz, total_ref,
                   wg, wu, wd, sem, s3, s4, r2, r3, r4, kept3, kept4, near, sq_ref, ssem, rsem, gsem_s, gsem_r, out_sem):
    me = lax.axis_index("dp")
    block = pl.program_id(0)
    sends, recvs, kepts = (s2, s3, s4), (r2, r3, r4), (kept2, kept3, kept4)
    wait = weights_in([wg_hbm.at[layer + 1], wu_hbm.at[layer + 1], wd_hbm.at[layer]], (wg, wu, wd), sem)

    def stage_copy(k, i):
        return pltpu.make_async_remote_copy(sends[k - 2].at[i], recvs[k - 2].at[i], ssem.at[k - 2, i], rsem.at[k - 2, i], **partner(me, k, in_order(i)))

    def gather_copy(k, i):
        c = in_order(i)
        rows = pl.ds(mult(offset(me, k, c) - offset(me, 1, c), 512 >> k), 512 >> k)
        return pltpu.make_async_remote_copy(near.at[c, rows], near.at[c, rows], gsem_s.at[k - 2, i], gsem_r.at[k - 2, i], **partner(me, k, c))

    @pl.when(block == 0)
    def _():
        meet(me, False)
        sq_ref[...] = jnp.zeros_like(sq_ref)

        def start(i):
            stage_copy(2, i).start()
        loop(0, CHUNKS, start)

    def stage_job(k, i):
        c = in_order(i)
        stage_copy(k, i).wait_recv()
        kept, got = kepts[k - 2], recvs[k - 2]
        if k == STAGES:
            out = (kept[i] + got[i].astype(F32)).astype(BF)
            wide = out.astype(F32)
            sq_ref[...] += wide * wide
            near[c, pl.ds(mult(offset(me, k, c) - offset(me, 1, c), 32), 32), :] = out
            gather_copy(STAGES, i).start()
            return
        give, keep = halves(me, k, c)
        sends[k - 1][i] = (kept[i, give, :] + got[i, give, :].astype(F32)).astype(BF)
        stage_copy(k + 1, i).start()
        kepts[k - 1][i] = kept[i, keep, :] + got[i, keep, :].astype(F32)

    def gather_job(k, i):
        gather_copy(k, i).wait_recv()
        if k > 2:
            gather_copy(k - 1, i).start()

    jobs = [functools.partial(stage_job, k) for k in range(2, STAGES + 1)] + [functools.partial(gather_job, k) for k in range(STAGES, 1, -1)]

    def attend(p):
        for lag, job in zip(POINT_LAGS, jobs):
            for r in range(RATE):
                i = RATE * (p - lag) + r

                @pl.when((i >= 0) & (i < CHUNKS))
                def _():
                    job(i)

    attend(block * POINTS)
    wait(0)
    by_gate = nt(dg1_ref[...], wg[...]).astype(BF).astype(F32)
    attend(block * POINTS + 1)
    wait(1)
    by_up = nt(du1_ref[...], wu[...]).astype(BF).astype(F32)
    attend(block * POINTS + 2)
    da = (by_gate + by_up).astype(BF).astype(F32)
    wide = h_ref[...].astype(F32)
    scale = lax.rsqrt(jnp.mean(wide * wide, -1, keepdims=True) + 1e-6)
    inner = jnp.mean(da * wide, -1, keepdims=True)
    dn = (da * scale - wide * (scale * scale * scale * inner)).astype(BF)
    dh = (dy_ref[0].astype(F32) + dn.astype(F32)).astype(BF)
    dht_ref[...] = dh.T
    wait(2)
    for c in range(0, wd.shape[0], CH):
        if c == 5 * CH:
            attend(block * POINTS + 3)
        cols = pl.ds(c, CH)
        ds = nt(dh, wd[cols, :]).astype(BF).astype(F32)
        dg_ref[:, cols] = (ds * fa_ref[:, cols]).astype(BF)
        du_ref[:, cols] = (ds * fb_ref[:, cols]).astype(BF)

    @pl.when(block == pl.num_programs(0) - 1)
    def _():
        first, stop = 2048 // ROWS * POINTS, (CHUNKS + RATE - 1) // RATE + POINT_LAGS[-1]

        def finish(p):
            attend(p)
        if stop > first:
            loop(first, stop, finish)

        def settle(i):
            for k in range(2, STAGES + 1):
                stage_copy(k, i).wait_send()
                gather_copy(k, i).wait_send()
        loop(0, CHUNKS, settle)
        total_ref[...] = squares_of(sq_ref)
        copies = [pltpu.make_async_copy(near.at[pl.ds(a, b - a)], g, out_sem.at[j]) for j, (a, b, g) in enumerate(zip(KINDS, KINDS[1:], (gx, gy, gz)))]
        for o in copies:
            o.start()
        for o in copies:
            o.wait()


def between_scratch():
    return [
        *[pltpu.VMEM((CHUNKS, n, CH), BF) for n in (64, 32, 128, 64, 32)],
        *[pltpu.VMEM((CHUNKS, n, CH), F32) for n in (64, 32)],
        pltpu.VMEM((CHUNKS, 256, CH), BF),
        pltpu.VMEM((32, CH), F32),
        *[pltpu.SemaphoreType.DMA((3, CHUNKS))] * 4,
        pltpu.SemaphoreType.DMA((3,)),
    ]


def clip(squares_ref):
    mean = jnp.sum(jnp.sum(squares_ref[...], 0, keepdims=True), 1, keepdims=True) * (1.0 / COUNT)
    return jnp.minimum(1.0, 0.5 * lax.rsqrt(mean + 1e-30))


def stepped(factor, w, m, v, g):
    g = g.astype(F32) * factor
    m = 0.9 * m + 0.1 * g
    v = 0.95 * v + 0.05 * g * g
    w = w.astype(F32)
    return (w - 0.02 * (m * lax.rsqrt(v + 1e-8) + 0.1 * w)).astype(BF), m, v


DEEP_IN, DEEP_OUT = 6, 4


def adam_kernel(layer, ranges, squares_ref, *refs):
    count = sum(len(pieces) for pieces in ranges)
    grads, refs = refs[: 3 * count], refs[3 * count :]
    ins = list(zip(refs[0:3], refs[3:6], refs[6:9]))
    outs, scratch = refs[-18:-9], refs[-9:]
    outs = list(zip(outs[0:3], outs[3:6], outs[6:9]))
    gb, ibufs, obufs, (isem, osem) = scratch[0], scratch[1:4], scratch[4:7], scratch[7:9]
    me = lax.axis_index("dp")
    per, many = CHUNKS // 3, len(ranges)
    factor = clip(squares_ref)

    def holder(piece, c):
        device = me
        for stage in piece:
            device = partner_of(device, bit_of(int(stage), c))
        return device

    def base_of(i):
        c, row = i // many, 0
        for r, pieces in enumerate(ranges):
            device = holder(pieces[0], c)
            at = side_of(device, 1) * 512 + offset(device, 1, c)
            row = jnp.where(i % many == r, at, row)
        return mult(row, 256)

    def blocks(i, groups, act):
        c, row = i // many, base_of(i)
        for matrix in range(3):
            @pl.when(c // per == (matrix + 1) % 3)
            def _():
                hidden = pl.ds(mult((c % per) * CH, CH), CH)
                at = (layer, hidden, pl.ds(row, 256)) if matrix == 2 else (layer, pl.ds(row, 256), hidden)
                for k, ref in enumerate(groups[matrix]):
                    act(ref.at[at], k)

    def reads(i, act):
        slot, c = i % DEEP_IN, i // many
        at = 0
        for r, pieces in enumerate(ranges):
            for kind in range(3):
                @pl.when((i % many == r) & (c >= KINDS[kind]) & (c < KINDS[kind + 1]))
                def _():
                    for j, piece in enumerate(pieces):
                        rows = 256 // len(pieces)
                        row = side_of(holder(piece, c), bit_of(2, c)) * rows if len(pieces) == 2 else 0
                        act(grads[3 * (at + j) + kind].at[c - KINDS[kind]], gb.at[slot, pl.ds(mult(row, rows), rows)], isem.at[3 + j, slot])
            at += len(pieces)
        blocks(i, ins, lambda ref, k: act(ref, ibufs[k].at[slot], isem.at[k, slot]))

    def writes(i, act):
        slot = i % DEEP_OUT
        blocks(i, outs, lambda ref, k: act(obufs[k].at[slot], ref, osem.at[k, slot]))

    def compute(i):
        a, b = i % DEEP_IN, i % DEEP_OUT

        def update(turned):
            for q in range(0, 256, 128):
                at = (pl.ds(q, 128), slice(None))
                g = gb[a, :, pl.ds(q, 128)].T if turned else gb[a, *at]
                new = stepped(factor, *(buf[a, *at] for buf in ibufs), g)
                for buf, value in zip(obufs, new):
                    buf[b, *at] = value

        @pl.when(i // many < per)
        def _():
            update(True)

        @pl.when(i // many >= per)
        def _():
            update(False)

    def each(copies, i, act):
        copies(i, lambda src, dst, sem: getattr(pltpu.make_async_copy(src, dst, sem), act)())

    steps = CHUNKS * many
    for i in range(DEEP_IN - 1):
        each(reads, jnp.int32(i), "start")

    def step(i):
        @pl.when(i + DEEP_IN - 1 < steps)
        def _():
            each(reads, i + DEEP_IN - 1, "start")
        each(reads, i, "wait")

        @pl.when(i >= DEEP_OUT)
        def _():
            each(writes, i - DEEP_OUT, "wait")
        compute(i)
        each(writes, i, "start")

    loop(0, steps, step)

    def settle(i):
        each(writes, i, "wait")
    loop(steps - DEEP_OUT, steps, settle)


def adam(name, layer, ranges, squares, pieces, arrays, before):
    grads = [a for r in ranges for piece in r for a in pieces[piece]]
    kinds = (BF, F32, F32)
    size = CHUNKS * len(ranges) * 256 * CH
    return pl.pallas_call(
        functools.partial(adam_kernel, layer, ranges),
        in_specs=[VMEM] + [ANY] * (len(grads) + len(arrays) + len(before)),
        out_specs=[ANY] * len(arrays),
        out_shape=[struct(a.dtype, *a.shape) for a in arrays],
        scratch_shapes=[pltpu.VMEM((DEEP_IN, 256, CH), kind) for kind in (BF, *kinds)] + [pltpu.VMEM((DEEP_OUT, 256, CH), kind) for kind in kinds]
        + [pltpu.SemaphoreType.DMA((5, DEEP_IN)), pltpu.SemaphoreType.DMA((3, DEEP_OUT))],
        input_output_aliases={1 + len(grads) + len(arrays) + i: i for i in range(len(before))},
        compiler_params=pltpu.CompilerParams(vmem_limit_bytes=60 * MiB),
        cost_estimate=pl.CostEstimate(flops=3000 * size, bytes_accessed=22 * size, transcendentals=0),
        name=name,
    )(squares, *grads, *arrays, *before)


def across(stage, kinds):
    bits = ((1, 1, 1), (16, 8, 2), (8, 16, 4))[stage]
    return [lax.ppermute(a, "dp", [(i, i ^ bit) for i in range(32)]) for a, bit in zip(kinds, bits, strict=True)]


def together(*groups):
    flat = lax.optimization_barrier(tuple(a for g in groups for a in g))
    out = []
    for g in groups:
        out.append(list(flat[: len(g)]))
        flat = flat[len(g) :]
    return out


def solution(mesh):
    def step(x, dy, *arrays):
        weights = arrays[:3]
        layers, d, ff = weights[0].shape
        t = x.shape[1]
        wide, tall, flat = struct(BF, t, ff), struct(BF, d, t), struct(BF, t, d)
        s0, fa, fb, a0t, h1 = row_local(functools.partial(forward_kernel, 0), "fwd0", [x], weights,
                                        [wide, struct(F32, t, ff), struct(F32, t, ff), tall, flat], 3)
        s1, dg1, du1, a1t, dyt = row_local(functools.partial(top_kernel, 1), "top", [h1, dy], weights, [wide, wide, wide, tall, tall], 3)
        halved = begun(dyt, a1t, s1, dg1, du1, 1)
        dg0, du0, dht, *near1, sq1 = row_local(
            functools.partial(between_kernel, 0), "between", [dg1, du1, h1, dy, fa, fb], weights, [wide, wide, tall], 3,
            whole=halved, free=[*by_kind(256), struct(F32, 8, 128)], scratch=between_scratch(), cid=3)
        one, zero = {}, {}
        one["0"] = across(0, near1)
        *zero[""], squares = summed(dht, a0t, s0, dg0, du0, sq1, 2)
        one["0"], zero[""], one[""], (squares,) = together(one["0"], zero[""], near1, (squares,))
        one["1"] = across(1, one[""])
        for stage, piece in enumerate("02"):
            zero[piece] = across(2 * stage, zero[""])
        new = adam("adam1a", 1, [[""], ["0"]], squares, one, arrays, ())
        new, one["1"] = together(new, one["1"])
        one["01"] = across(0, one["1"])
        new = adam("adam1b", 1, [["1"]], squares, one, arrays, new)
        new, zero["2"], zero["0"], one["01"] = together(new, zero["2"], zero["0"], one["01"])
        zero["1"] = across(1, zero[""])
        zero["12"] = across(1, zero["2"])
        zero["02"] = across(0, zero["2"])
        new = adam("adam1c", 1, [["01"]], squares, one, arrays, new)
        new, zero["02"] = together(new, zero["02"])
        new = adam("adam0a", 0, [["", "2"], ["0", "02"]], squares, zero, arrays, new)
        new, zero["1"], zero["12"] = together(new, zero["1"], zero["12"])
        for piece in ("1", "12"):
            zero["0" + piece] = across(0, zero[piece])
        new = adam("adam0b", 0, [["1", "12"]], squares, zero, arrays, new)
        new, zero["01"], zero["012"] = together(new, zero["01"], zero["012"])
        return tuple(adam("adam0c", 0, [["01", "012"]], squares, zero, arrays, new))

    return jax.shard_map(
        step,
        mesh=mesh,
        in_specs=(P(("rep", "dp")),) * 2 + (P(),) * 9,
        out_specs=(P("rep"),) * 9,
        check_vma=False,
    )
```
